32 devices in a mesh: wide: 8 (over z, y), narrow: 4 (over x, core).
Axes of the slice: x: 2, y: 2, z: 4, core: 2. Of those that a mesh axis runs over, the one named last changes fastest.
Arguments:
- targets: float32 [32768, 64], P(('wide', 'narrow')), may hold values from -6 to 6
- train_features: bfloat16 [32768, 128], P(('wide', 'narrow')), may hold values from -6 to 6
- test_features: bfloat16 [1024, 128], P(('wide', 'narrow')), may hold values from -6 to 6
- left_factors: float32 [32768, 4, 128], P(('wide', 'narrow')), may hold values from -0.5 to 0.5
- right_factors: float32 [32768, 4, 128], P(('wide', 'narrow')), may hold values from -0.03125 to 0.03125
- capacitance: float32 [15, 256, 256], replicated, may hold values from -0.375 to 0.375
- pivots: int32 [15, 256], replicated, may hold values from 0 to 255, each once within a row
Outputs:
- solved_targets: float32 [32768, 64], P(('wide', 'narrow'))
- predictions: float32 [1024, 64], P(('wide', 'narrow'))
The draws below stay inside these ranges and needn't reach their ends.
Inputs may be any that keep to these rules, and one draw needn't show every extreme that they name: `pivots`: each row is a permutation of 0 .. 255.
All inputs are finite; a program needn't handle non-finite values.
Results may differ from the reference program's by a relative error of at most 0.0049.
Values may be sent and summed in bfloat16 or wider, within the bound.
A program may use at most 128 MiB of HBM per device.

```python
import jax
import jax.numpy as jnp
from jax import lax

R = 128
FEAT = 128
TARGETS = 64
LEVELS = 4
NODES = 15
POINTS = 32768
TESTS = 1024


def steps_of(own_key, extent, pieces, low, top_value):
    factor_of = 1.0
    for dim, shards_of in pieces:
        steps = jax.random.uniform(jax.random.fold_in(jax.random.fold_in(own_key, 6), dim), (shards_of,), jnp.float32, low / len(pieces), top_value / len(pieces))
        factor_of = factor_of * jnp.repeat(jnp.exp(steps), extent[dim] // shards_of).reshape((-1,) + (1,) * (len(extent) - 1 - dim))
    return factor_of


def bell_draw(own_key, extent, scale, most, shards=(), kind=jnp.bfloat16):
    entries = jax.random.normal(own_key, extent, jnp.float32) * scale
    if len(shards) > 0:
        entries = steps_of(own_key, extent, shards, -0.22, 0.18) * entries
    return jnp.clip(entries, min=-most, max=most).astype(kind)


def setup_inputs(seed: int = 0) -> dict:
    key_of = jax.random.split(jax.random.key(seed), 8)
    return {
        "targets": bell_draw(key_of[0], (POINTS, TARGETS), 1.0, 6.0, ((0, 32),), jnp.float32),
        "train_features": bell_draw(key_of[1], (POINTS, FEAT), 1.0, 6.0, ((0, 32),)),
        "test_features": bell_draw(key_of[2], (TESTS, FEAT), 1.0, 6.0, ((0, 32),)),
        "left_factors": bell_draw(key_of[3], (POINTS, LEVELS, R), R ** -0.5, 0.5, ((0, 32),), jnp.float32),
        "right_factors": bell_draw(key_of[4], (POINTS, LEVELS, R), POINTS ** -0.5, 0.03125, ((0, 32),), jnp.float32),
        "capacitance": bell_draw(key_of[5], (NODES, 2 * R, 2 * R), (2 * R) ** -0.5, 0.375, (), jnp.float32),
        "pivots": jax.vmap(lambda own: jax.random.permutation(own, 2 * R))(jax.random.split(key_of[6], NODES)).reshape((NODES, 2 * R)).astype(jnp.int32),
    }


spread_coef = 3.0


def level_update(current, left_level, right_level, capacitance, pivots, tree_level):
    children = 2 ** tree_level
    nodes = children // 2
    offset = nodes - 1
    per_child = POINTS // children
    right_blocks = right_level.reshape(children, per_child, R)
    left_blocks = left_level.reshape(children, per_child, R)
    value_blocks = current.reshape(children, per_child, TARGETS)
    projected = jnp.einsum("cpr,cpt->crt", right_blocks, value_blocks, precision=lax.Precision.HIGHEST)
    paired = projected.reshape(nodes, 2, R, TARGETS)
    stacked = jnp.concatenate([paired[:, 1], paired[:, 0]], axis=1)
    node_pivots = pivots[offset:offset + nodes].astype(jnp.int32)
    permuted = jnp.take_along_axis(stacked, node_pivots[:, :, None], axis=1)
    caps = capacitance[offset:offset + nodes]
    solved = jnp.einsum("nij,njt->nit", caps, permuted, precision=lax.Precision.HIGHEST)
    shares = solved.reshape(children, R, TARGETS)
    update = jnp.einsum("cpr,crt->cpt", left_blocks, shares, precision=lax.Precision.HIGHEST)
    return current - update.reshape(POINTS, TARGETS)


def reference(targets, train_features, test_features, left_factors, right_factors, capacitance, pivots):
    current = targets.astype(jnp.float32)
    for tree_level in range(1, LEVELS + 1):
        current = level_update(current, left_factors[:, tree_level - 1, :], right_factors[:, tree_level - 1, :], capacitance, pivots, tree_level)
    weights_bf = current.astype(jnp.bfloat16)
    train_float = train_features.astype(jnp.float32)
    train_sq = jnp.sum(train_float * train_float, axis=1)
    block_rows = 128 if TESTS % 128 == 0 else TESTS
    blocks = test_features.reshape(TESTS // block_rows, block_rows, FEAT)

    def predict_block(rows_in):
        rows_float = rows_in.astype(jnp.float32)
        row_sq = jnp.sum(rows_float * rows_float, axis=1)
        inner = lax.dot_general(rows_in, train_features, (((1,), (1,)), ((), ())), preferred_element_type=jnp.float32)
        dist = row_sq[:, None] + train_sq[None, :] - 2.0 * inner
        kernel = jnp.exp(-(spread_coef / FEAT) * dist).astype(jnp.bfloat16)
        return jnp.dot(kernel, weights_bf, preferred_element_type=jnp.float32)

    predictions = lax.map(predict_block, blocks).reshape(TESTS, TARGETS)
    return current, predictions
```

```python
import functools

import jax
import jax.numpy as jnp
from jax import lax
from jax.experimental import pallas as pl
from jax.experimental.pallas import tpu as pltpu
from jax.sharding import PartitionSpec as P

LEVELS = 4
spread_coef = 3.0
MESH = pl.DeviceIdType.MESH
HIGHEST = lax.Precision.HIGHEST


def dot(a, b, precision=None):
    return jnp.dot(a, b, precision=precision, preferred_element_type=jnp.float32)


def dot_nt(a, b, precision=None):
    return lax.dot_general(
        a, b, (((1,), (1,)), ((), ())), precision=precision, preferred_element_type=jnp.float32
    )


def split(value):
    high = value.astype(jnp.bfloat16)
    return high, (value - high.astype(jnp.float32)).astype(jnp.bfloat16)


def g_row(level, k, rank):
    return ((level - 1) * (level - 2) // 2 + (k - 1)) * rank


def kernel(
    n_dev, narrow,
    targets_h, train_h, test_h, left_h, right_h, cap_h, piv_ref,
    cur_ref, pred_ref,
    tgt, train, left, right, cap, gath, lsplit, mt, kmat,
    acc_t, acc_g, par_t, par_g, send_t, send_g, recv_t, recv_g,
    share, term_f, term_b, term_in,
    load_sem, cap_sem, t1_send, t1_recv, tt_send, tt_recv, gg_send, gg_recv,
    ag_send, ag_recv, fw_send, fw_recv, rs_send, rs_recv,
):
    bits = n_dev.bit_length() - 1
    pos = lax.axis_index("wide") * narrow + lax.axis_index("narrow")
    points, width = tgt.shape
    rank = right.shape[2]
    feat = train.shape[1]
    rows = test_h.shape[0]
    half = rows // 2
    parity = pos % 2
    slot = pos // 2
    pairs = n_dev // 2

    def coords(dev):
        return (dev // narrow, dev % narrow)

    barrier = pltpu.get_barrier_semaphore()

    def greet(k, carry):
        pl.semaphore_signal(
            barrier, inc=1, device_id=coords((pos + k) % n_dev), device_id_type=MESH
        )
        return carry

    lax.fori_loop(1, n_dev, greet, 0)

    own_test = gath.at[parity, pl.ds(pl.multiple_of(slot * rows, rows), rows)]
    loads = [
        pltpu.make_async_copy(targets_h, tgt, load_sem.at[0]),
        pltpu.make_async_copy(train_h, train, load_sem.at[1]),
        pltpu.make_async_copy(test_h, own_test, load_sem.at[2]),
    ]
    for lev in range(LEVELS):
        loads.append(pltpu.make_async_copy(right_h.at[:, lev, :], right.at[lev], load_sem.at[3 + lev]))
        loads.append(
            pltpu.make_async_copy(left_h.at[:, lev, :], left.at[lev], load_sem.at[3 + LEVELS + lev])
        )
    caps = []
    odds, heaps = [], []
    for level in range(1, LEVELS + 1):
        child = pos // (n_dev >> level)
        odds.append(child % 2)
        heaps.append((1 << level - 1) - 1 + child // 2)
        caps.append(
            pltpu.make_async_copy(
                cap_h.at[heaps[-1], pl.ds(pl.multiple_of(odds[-1] * rank, rank), rank)],
                cap.at[level - 1],
                cap_sem.at[level - 1],
            )
        )
    for copy in loads + caps:
        copy.start()
    for copy in loads:
        copy.wait()

    tgt_high, tgt_low = split(tgt[...].T)
    stack = [tgt_high, tgt_low]
    for lev in range(LEVELS - 1):
        stack.append(left[lev].T.astype(jnp.bfloat16))
    for level in range(1, LEVELS + 1):
        right_high, right_low = split(right[level - 1])
        product = dot(jnp.concatenate(stack[: 1 + level], axis=0), right_high)
        acc_t[pl.ds((level - 1) * width, width)] = (
            product[:width] + product[width : 2 * width] + dot(tgt_high, right_low)
        )
        if level > 1:
            acc_g[pl.ds(g_row(level, 1, rank), (level - 1) * rank)] = product[2 * width :]

    def partner_of(bit):
        mask = 1 << bit
        return coords(pos + mask * (1 - 2 * ((pos // mask) % 2)))

    def levels_at(bit):
        return min(LEVELS, bits - bit)

    def t1_copy(bit):
        part = pl.ds(0, width)
        return pltpu.make_async_remote_copy(
            src_ref=send_t.at[bit, part], dst_ref=recv_t.at[bit, part],
            send_sem=t1_send.at[bit], recv_sem=t1_recv.at[bit],
            device_id=partner_of(bit), device_id_type=MESH,
        )

    def tt_copy(bit):
        part = pl.ds(width, (levels_at(bit) - 1) * width)
        return pltpu.make_async_remote_copy(
            src_ref=send_t.at[bit, part], dst_ref=recv_t.at[bit, part],
            send_sem=tt_send.at[bit], recv_sem=tt_recv.at[bit],
            device_id=partner_of(bit), device_id_type=MESH,
        )

    def gg_copy(bit):
        part = pl.ds(0, g_row(levels_at(bit) + 1, 1, rank))
        return pltpu.make_async_remote_copy(
            src_ref=send_g.at[bit, part], dst_ref=recv_g.at[bit, part],
            send_sem=gg_send.at[bit], recv_sem=gg_recv.at[bit],
            device_id=partner_of(bit), device_id_type=MESH,
        )

    def send_first(bit):
        part = pl.ds(0, width)
        send_t[bit, part] = acc_t[part]
        t1_copy(bit).start()

    def send_rest(bit):
        if levels_at(bit) > 1:
            part = pl.ds(width, (levels_at(bit) - 1) * width)
            send_t[bit, part] = acc_t[part]
            tt_copy(bit).start()
            part = pl.ds(0, g_row(levels_at(bit) + 1, 1, rank))
            send_g[bit, part] = acc_g[part].astype(jnp.bfloat16)
            gg_copy(bit).start()

    def take_first(bit):
        t1_copy(bit).wait()
        part = pl.ds(0, width)
        if bit < bits - 1:
            acc_t[part] = acc_t[part] + recv_t[bit, part]
        else:
            par_t[part] = recv_t[bit, part]

    def take_rest(bit):
        if levels_at(bit) == 1:
            return
        tt_copy(bit).wait()
        gg_copy(bit).wait()
        top = bits - bit
        summed = min(LEVELS, top - 1)
        if summed > 1:
            part = pl.ds(width, (summed - 1) * width)
            acc_t[part] = acc_t[part] + recv_t[bit, part]
            part = pl.ds(0, g_row(summed + 1, 1, rank))
            acc_g[part] = acc_g[part] + recv_g[bit, part].astype(jnp.float32)
        if top <= LEVELS:
            part = pl.ds((top - 1) * width, width)
            par_t[part] = recv_t[bit, part]
            part = pl.ds(g_row(top, 1, rank), (top - 1) * rank)
            par_g[part] = recv_g[bit, part].astype(jnp.float32)

    pl.semaphore_wait(barrier, n_dev - 1)
    send_first(0)
    send_rest(0)

    def spread(k, carry):
        dev = (pos + 2 * k) % n_dev
        pltpu.make_async_remote_copy(
            src_ref=own_test, dst_ref=own_test, send_sem=ag_send, recv_sem=ag_recv,
            device_id=coords(dev), device_id_type=MESH,
        ).start()
        return carry

    lax.fori_loop(1, pairs, spread, 0)

    for copy in caps:
        copy.wait()
    order = lax.broadcasted_iota(jnp.int32, (2 * rank, 2 * rank), 0)

    def pivot(lev):
        chosen = (order == piv_ref[pl.ds(heaps[lev], 1), :]).astype(jnp.float32)
        mt[lev] = dot_nt(chosen, cap[lev], HIGHEST)

    def halves(lev):
        high, low = split(left[lev])
        lsplit[0, :, pl.ds(lev * rank, rank)] = high
        lsplit[1, :, pl.ds(lev * rank, rank)] = low

    take_first(0)
    send_first(1)
    take_rest(0)
    send_rest(1)
    for lev in range(LEVELS):
        pivot(lev)

    def forward(which):
        part = gath.at[which]
        return pltpu.make_async_remote_copy(
            src_ref=part, dst_ref=part, send_sem=fw_send, recv_sem=fw_recv,
            device_id=partner_of(0), device_id_type=MESH,
        )

    def drain(ref, count, sem):
        part = ref.at[pl.ds(0, count)]
        pltpu.make_async_copy(part, part, sem).wait()

    scale = spread_coef / feat
    chunk = 128

    def kernel_rows(which):
        train_bf = train[...]
        train_f = train_bf.astype(jnp.float32)
        ones = jnp.ones((8, feat), jnp.float32)
        train_sq = dot_nt(ones, train_f * train_f, HIGHEST)[:1]

        def step(i, carry):
            part = pl.ds(pl.multiple_of(i * chunk, chunk), chunk)
            some = gath[which, part]
            some_f = some.astype(jnp.float32)
            some_sq = jnp.sum(some_f * some_f, axis=1, keepdims=True)
            dist = some_sq + train_sq - 2.0 * dot_nt(some, train_bf)
            kmat[which, part] = jnp.exp(-scale * dist).astype(jnp.bfloat16)
            return carry

        lax.fori_loop(0, pairs * rows // chunk, step, 0)

    for bit in range(1, bits):
        take_first(bit)
        if bit < bits - 1:
            send_first(bit + 1)
        if bit > 1:
            take_rest(bit - 1)
            send_rest(bit)
        if bit == 1:
            for lev in range(LEVELS):
                halves(lev)
        if bit == bits - 3:
            drain(gath.at[0], (pairs - 1) * rows, ag_recv)
            forward(parity).start()
            kernel_rows(parity)
        if bit == bits - 2:
            forward(parity).wait()
            kernel_rows(1 - parity)

    shares = []
    for level in range(1, LEVELS + 1):
        if level == 2 and bits > 1:
            take_rest(bits - 1)
        t_part = pl.ds((level - 1) * width, width)
        mine, other = acc_t[t_part], par_t[t_part]
        for k in range(1, level):
            g_part = pl.ds(g_row(level, k, rank), rank)
            mine = mine - dot(shares[k - 1], acc_g[g_part], HIGHEST)
            other = other - dot(shares[k - 1], par_g[g_part], HIGHEST)
        odd = odds[level - 1]
        at_mine = pl.ds(pl.multiple_of((1 - odd) * rank, rank), rank)
        at_other = pl.ds(pl.multiple_of(odd * rank, rank), rank)
        shares.append(
            dot(mine, mt[level - 1, at_mine], HIGHEST) + dot(other, mt[level - 1, at_other], HIGHEST)
        )
    share_high, share_low = split(jnp.concatenate(shares, axis=1))
    current = tgt[...] - (
        dot_nt(lsplit[0], share_high) + dot_nt(lsplit[1], share_high) + dot_nt(lsplit[0], share_low)
    )
    cur_ref[...] = current
    weights = current.astype(jnp.bfloat16)

    big = min(512, pairs * rows)
    for which in range(2):

        def weigh(i, carry, which=which):
            part = pl.ds(pl.multiple_of(i * big, big), big)
            terms = dot(kmat[which, part], weights).reshape(big // rows, 2, half, width)
            packed = jnp.concatenate(
                [terms[:, 0].reshape(big // 2, width), terms[:, 1].reshape(big // 2, width)], axis=1
            )
            term_b[which, pl.ds(pl.multiple_of(i * (big // 2), big // 2), big // 2)] = packed.astype(
                jnp.bfloat16
            )
            return carry

        lax.fori_loop(0, pairs * rows // big, weigh, 0)

    def scatter(k, carry):
        dev = (pos + k) % n_dev
        pltpu.make_async_remote_copy(
            src_ref=term_b.at[dev % 2, pl.ds(pl.multiple_of(dev // 2 * half, half), half)],
            dst_ref=term_in.at[pl.ds(pl.multiple_of((k - 1) * half, half), half)],
            send_sem=rs_send, recv_sem=rs_recv, device_id=coords(dev), device_id_type=MESH,
        ).start()
        return carry

    lax.fori_loop(1, n_dev, scatter, 0)
    drain(gath.at[0], (pairs - 1) * rows, ag_send)
    drain(term_in, (n_dev - 1) * half, rs_recv)
    total = term_b[parity, pl.ds(pl.multiple_of(slot * half, half), half)].astype(jnp.float32)
    arrived = term_in[...].astype(jnp.float32).reshape(n_dev - 1, half, 2 * width)
    total = total + jnp.sum(arrived, axis=0)
    pred_ref[pl.ds(0, half)] = total[:, :width]
    pred_ref[pl.ds(half, half)] = total[:, width:]
    drain(term_in, (n_dev - 1) * half, rs_send)


def body(n_dev, narrow, targets, train, test, left, right, cap, pivots):
    points, width = targets.shape
    rank = left.shape[2]
    feat = train.shape[1]
    rows = test.shape[0]
    bits = n_dev.bit_length() - 1
    pairs = n_dev // 2
    g_rows = g_row(LEVELS + 1, 1, rank)
    t_rows = LEVELS * width
    f32, bf16 = jnp.float32, jnp.bfloat16
    vmem = pltpu.VMEM
    dma = pltpu.SemaphoreType.DMA
    hbm_spec = pl.BlockSpec(memory_space=pl.ANY)
    vmem_spec = pl.BlockSpec(memory_space=pltpu.VMEM)
    return pl.pallas_call(
        functools.partial(kernel, n_dev, narrow),
        out_shape=(
            jax.ShapeDtypeStruct((points, width), f32),
            jax.ShapeDtypeStruct((rows, width), f32),
        ),
        in_specs=[hbm_spec] * 6 + [vmem_spec],
        out_specs=(vmem_spec, vmem_spec),
        scratch_shapes=[
            vmem((points, width), f32),
            vmem((points, feat), bf16),
            vmem((LEVELS, points, rank), f32),
            vmem((LEVELS, points, rank), f32),
            vmem((LEVELS, rank, 2 * rank), f32),
            vmem((2, pairs * rows, feat), bf16),
            vmem((2, points, LEVELS * rank), bf16),
            vmem((LEVELS, 2 * rank, rank), f32),
            vmem((2, pairs * rows, points), bf16),
            vmem((t_rows, rank), f32),
            vmem((g_rows, rank), f32),
            vmem((t_rows, rank), f32),
            vmem((g_rows, rank), f32),
            vmem((bits, t_rows, rank), f32),
            vmem((bits, g_rows, rank), bf16),
            vmem((bits, t_rows, rank), f32),
            vmem((bits, g_rows, rank), bf16),
            vmem((8, 128), f32),
            vmem((8, 128), f32),
            vmem((2, pairs * rows // 2, 2 * width), bf16),
            vmem(((n_dev - 1) * rows // 2, 2 * width), bf16),
            dma((3 + 2 * LEVELS,)),
            dma((LEVELS,)),
            dma((bits,)), dma((bits,)), dma((bits,)), dma((bits,)), dma((bits,)), dma((bits,)),
            dma, dma, dma, dma, dma, dma,
        ],
        compiler_params=pltpu.CompilerParams(
            collective_id=0, has_side_effects=True, vmem_limit_bytes=60 * 1024 * 1024
        ),
    )(targets, train, test, left, right, cap, pivots)


def solution(mesh):
    both = ("wide", "narrow")
    placed = (
        P(both, None), P(both, None), P(both, None),
        P(both, None, None), P(both, None, None), P(), P(),
    )
    sizes = dict(mesh.shape)
    return jax.shard_map(
        functools.partial(body, sizes["wide"] * sizes["narrow"], sizes["narrow"]),
        mesh=mesh,
        in_specs=placed,
        out_specs=(P(both, None), P(both, None)),
        check_vma=False,
    )
```
